32 devices in a mesh: samp: 8 (over z, x), feat: 4 (over y, core).
Axes of the slice: x: 2, y: 2, z: 4, core: 2. Of those that a mesh axis runs over, the one named last changes fastest.
Arguments:
- inputs: bfloat16 [16384, 96], P('samp'), may hold values from -6 to 6
- frequencies: bfloat16 [96, 16384], P(None, 'feat'), may hold values from -0.625 to 0.625
- phases: float32 [16384], P('feat'), may hold values from -3.140625 to 3.140625
- targets: float32 [16384], P('samp'), may hold values from -12 to 12
- block_order: int32 [16384], P('samp'), may hold values from 0 to 2047, as said below
Outputs:
- weights: float32 [16384], P('feat')
- duals: float32 [16384], P('samp')
- objectives: float32 [4, 2], replicated
The draws below stay inside these ranges and needn't reach their ends.
Inputs may be any that keep to these rules, and one draw needn't show every extreme that they name: `block_order`: within each aligned run of 2048 samples, a permutation of 0 to 2047.
All inputs are finite; a program needn't handle non-finite values.
Results may differ from the reference program's by a relative error of at most 0.0054.
The reference program's roundings to bfloat16 on the way count: a program that leaves them out, or rounds other values in their place, can miss the bound.
Values may be sent and summed in bfloat16 or wider, within the bound.
A program may use at most 64 MiB of HBM per device.

```python
import math
import jax
import jax.numpy as jnp
from jax import lax

FEATURES = 16384
INPUTS = 96
BLOCK = 256
BLOCKS_DEV = 8
ROUNDS = 4
SAMPLES = 16384
N_SAMP = 8


def draw_targets(key, part):
    index = jnp.arange(SAMPLES, dtype=jnp.float32)
    ramp = 1.0 + 2.0 * index / (SAMPLES - 1)
    base = jnp.clip(jax.random.normal(key, (SAMPLES,), jnp.float32), -4.0, 4.0)
    values = base * ramp
    return values.astype(jnp.float32)


def draw_block_order(key, part):
    row_count = BLOCKS_DEV * BLOCK
    groups = SAMPLES // row_count
    keys = jax.random.split(jax.random.fold_in(key, 7), groups)
    perms = jax.vmap(lambda single: jax.random.permutation(single, row_count))(keys)
    return perms.reshape(SAMPLES).astype(jnp.int32)


def level_of(stream_key, shape, cuts, low, largest):
    loudness = 1.0
    for axis_at, parts in cuts:
        steps = jax.random.uniform(jax.random.fold_in(jax.random.fold_in(stream_key, 6), axis_at), (parts,), jnp.float32, low / len(cuts), largest / len(cuts))
        loudness = loudness * jnp.repeat(jnp.exp(steps), shape[axis_at] // parts).reshape((-1,) + (1,) * (len(shape) - 1 - axis_at))
    return loudness


def noise(key, extent, width, most, pieces=(), kind=jnp.bfloat16):
    loudness = level_of(key, extent, pieces, -0.22, 0.18) if pieces else 1.0
    values = jax.random.normal(key, extent, jnp.float32) * width * loudness
    return jnp.minimum(jnp.maximum(values, -most), most).astype(kind)


def setup_inputs(seed: int = 0) -> dict:
    seeds = jax.random.split(jax.random.key(seed), 6)
    return {
        "inputs": noise(seeds[0], (SAMPLES, INPUTS), 1.0, 6.0, ((0, 8),)),
        "frequencies": noise(seeds[1], (INPUTS, FEATURES), INPUTS ** -0.5, 0.625, ((1, 4),)),
        "phases": jnp.clip(jax.random.uniform(seeds[2], (FEATURES,), jnp.float32, -3.140625, 3.140625), -3.140625, 3.140625),
        "targets": draw_targets(jax.random.fold_in(seeds[5], 71), 0),
        "block_order": draw_block_order(jax.random.fold_in(seeds[5], 71), 0),
    }


highest = lax.Precision.HIGHEST

def feature_block(inputs_part, order_part, frequencies, phases):
    picked = inputs_part[order_part]
    angles = jnp.dot(picked.astype(jnp.float32), frequencies.astype(jnp.float32), precision=highest)
    return (math.sqrt(2.0 / FEATURES) * jnp.cos(angles + phases)).astype(jnp.bfloat16)

def solve_block(factor, vector):
    return jax.scipy.linalg.cho_solve((factor, True), vector)

def reference(inputs, frequencies, phases, targets, block_order):
    row_count = BLOCKS_DEV * BLOCK
    groups = N_SAMP
    ridge = 1.0 / BLOCK
    step_scale = BLOCK / SAMPLES
    inputs_grouped = inputs.reshape(groups, row_count, INPUTS)
    order_grouped = block_order.reshape(groups, row_count)
    wanted = jnp.take_along_axis(targets.reshape(groups, row_count), order_grouped, axis=1)

    def make_factor(pair):
        features = feature_block(pair[0], pair[1], frequencies, phases).astype(jnp.float32)
        features = features.reshape(BLOCKS_DEV, BLOCK, FEATURES)
        gram = jnp.einsum('bid,bjd->bij', features, features, precision=highest)
        return jnp.linalg.cholesky(gram + jnp.eye(BLOCK, dtype=jnp.float32))
    factors = lax.map(make_factor, (inputs_grouped, order_grouped))
    duals = jnp.zeros((groups, row_count), jnp.float32)
    margins = jnp.zeros((groups, row_count), jnp.float32)
    weights = jnp.zeros((FEATURES,), jnp.float32)
    records = []
    for round_index in range(ROUNDS):
        residual = (wanted - duals - margins).reshape(groups, BLOCKS_DEV, BLOCK)
        update = jax.vmap(jax.vmap(solve_block))(factors, residual).reshape(groups, row_count)
        duals = duals + update
        update_bf = lax.optimization_barrier(update.astype(jnp.bfloat16))

        def contribution(triple):
            features = feature_block(triple[0], triple[1], frequencies, phases).astype(jnp.float32)
            return jnp.dot(triple[2].astype(jnp.float32), features, precision=highest) * step_scale
        weights = weights + lax.optimization_barrier(jnp.sum(lax.map(contribution, (inputs_grouped, order_grouped, update_bf)), axis=0))
        weight_bf = lax.optimization_barrier(weights.astype(jnp.bfloat16)).astype(jnp.float32)

        def margin_block(pair):
            features = feature_block(pair[0], pair[1], frequencies, phases).astype(jnp.float32)
            return jnp.dot(features, weight_bf, precision=highest)
        margins = lax.map(margin_block, (inputs_grouped, order_grouped))
        squares = jnp.sum((margins - wanted) ** 2)
        dual_sum = jnp.sum(duals * wanted - 0.5 * duals * duals)
        norm_value = jnp.sum(weights * weights)
        records.append(jnp.stack([squares / (2.0 * SAMPLES) + 0.5 * ridge * norm_value, dual_sum / SAMPLES - 0.5 * ridge * norm_value]))
    objectives = jnp.stack(records)
    restored = jax.vmap(lambda values, order_part: jnp.zeros_like(values).at[order_part].set(values))(duals, order_grouped)
    return (weights, restored.reshape(SAMPLES), objectives)
```

```python
import functools
import math

import jax
import jax.numpy as jnp
import numpy as np
from jax import lax
from jax.experimental import pallas as pl
from jax.experimental.pallas import tpu as pltpu
from jax.sharding import PartitionSpec as P

FEATURES = 16384
BLOCK = 256
ROUNDS = 4
LANES = 128
CHUNK = 512
MESH = pl.DeviceIdType.MESH
F32 = jnp.float32
BF16 = jnp.bfloat16


def cosine_coefficients():
    nodes = np.cos((np.arange(400) + 0.5) * np.pi / 400)
    square = (nodes + 1.0) / 8.0
    values = math.sqrt(2.0 / FEATURES) * np.cos(2.0 * np.pi * np.sqrt(square))
    fit = np.polynomial.chebyshev.Chebyshev.fit(square, values, 5, domain=[0.0, 0.25])
    return [float(c) for c in fit.convert(kind=np.polynomial.Polynomial).coef]


COEFS = cosine_coefficients()


def nn(a, b, precision=None):
    return lax.dot_general(a, b, (((1,), (0,)), ((), ())), precision=precision, preferred_element_type=F32)


def nt(a, b):
    return lax.dot_general(a, b, (((1,), (1,)), ((), ())), preferred_element_type=F32)


def halves(a):
    high = a.astype(BF16)
    return high, (a - high.astype(F32)).astype(BF16)


def thirds(a):
    high = a.astype(BF16)
    rest = a - high.astype(F32)
    middle = rest.astype(BF16)
    return high, middle, (rest - middle.astype(F32)).astype(BF16)


def mm3(a, b):
    a_high, a_low = halves(a)
    b_high, b_low = halves(b)
    return nn(a_high, b_high) + (nn(a_high, b_low) + nn(a_low, b_high))


def mm6(a, b):
    return nn(a, b, lax.Precision.HIGHEST)


def stacked(row):
    high, middle, low = (piece.astype(F32) for piece in thirds(row))
    at = lax.broadcasted_iota(jnp.int32, (8, row.shape[1]), 0)
    return jnp.where(at == 0, high, jnp.where(at == 1, middle, low)).astype(BF16)


def unstacked(rows):
    return rows[0:1] + rows[1:2] + rows[2:3]


def kernel(n_samp, n_feat, inputs, freqs, phases, targets, order, w_out, duals_out, obj_out,
           phi, onehot, wanted, duals, margins, weights, w_wide, d_col, y, gram, gram_in, inverse,
           d_buf, w_buf, m_send, m_buf, s_feat, s_samp,
           g_ssem, g_rsem, d_ssem, d_rsem, w_ssem, w_rsem, m_ssem, m_rsem, f_ssem, f_rsem, t_ssem, t_rsem):
    samp, feat = lax.axis_index("samp"), lax.axis_index("feat")
    rows, width = phi.shape
    blocks = rows // BLOCK
    own = blocks // n_feat
    sample_total = rows * n_samp
    ridge = 1.0 / BLOCK
    step_scale = BLOCK / sample_total
    first = feat * own

    barrier = pltpu.get_barrier_semaphore()
    for k in range(1, n_feat):
        pl.semaphore_signal(barrier, inc=1, device_id=(samp, (feat + k) % n_feat), device_id_type=MESH)
    for k in range(1, n_samp):
        pl.semaphore_signal(barrier, inc=1, device_id=((samp + k) % n_samp, feat), device_id_type=MESH)
    pl.semaphore_wait(barrier, n_feat + n_samp - 2)

    def to_feat(peer, src, dst, ssem, rsem):
        return pltpu.make_async_remote_copy(src_ref=src, dst_ref=dst, send_sem=ssem, recv_sem=rsem,
                                            device_id=(samp, peer), device_id_type=MESH)

    def to_samp(peer, src, dst, ssem, rsem):
        return pltpu.make_async_remote_copy(src_ref=src, dst_ref=dst, send_sem=ssem, recv_sem=rsem,
                                            device_id=(peer, feat), device_id_type=MESH)

    target_rows = stacked(targets[...])

    half = n_feat // 2
    chip, core = feat // 2, feat % 2

    def owner_of(k):
        return ((chip + 1 + k // 2) % half) * 2 + (core + 1 + k % 2) % 2

    def gram_copy(i):
        peer = owner_of(i // own)
        local = i % own
        return to_feat(peer, gram.at[peer * own + local], gram_in.at[feat, local],
                       g_ssem.at[peer, local], g_rsem.at[feat, local])

    def make_block(i, carry):
        block = owner_of(i // own) * own + i % own
        at = pl.ds(pl.multiple_of(block * BLOCK, BLOCK), BLOCK)
        position = lax.broadcasted_iota(jnp.int32, (BLOCK, rows), 1)
        hot = jnp.where(order[at, :] == position, 1.0, 0.0).astype(BF16)
        onehot[at, :] = hot
        wanted[block] = unstacked(nt(target_rows, hot))
        picked = nn(hot, inputs[...]).astype(BF16)
        total = None
        for c in range(0, width, CHUNK):
            turns = nn(picked, freqs[:, c:c + CHUNK]) + phases[:, c:c + CHUNK]
            turns = turns * (0.5 / math.pi)
            turns = turns - jnp.floor(turns + 0.5)
            square = turns * turns
            value = COEFS[5] * square + COEFS[4]
            for coef in COEFS[3::-1]:
                value = value * square + coef
            part = value.astype(BF16)
            phi[at, c:c + CHUNK] = part
            term = nt(part, part)
            total = term if total is None else total + term

        @pl.when(i < blocks - own)
        def _():
            gram[block] = total
            gram_copy(i).start()

        @pl.when(i >= blocks - own)
        def _():
            gram_in[feat, i % own] = total

        return carry

    lax.fori_loop(0, blocks, make_block, 0)
    for i in range(blocks - own):
        peer = (feat + 1 + i // own) % n_feat
        copy = to_feat(peer, gram.at[peer * own + i % own], gram_in.at[peer, i % own],
                       g_ssem.at[peer, i % own], g_rsem.at[peer, i % own])
        copy.wait_recv()
        copy.wait_send()

    eye = jnp.where(lax.broadcasted_iota(jnp.int32, (BLOCK, BLOCK), 0)
                    == lax.broadcasted_iota(jnp.int32, (BLOCK, BLOCK), 1), 1.0, 0.0).astype(F32)
    lows = []
    for local in range(own):
        matrix = eye
        for k in range(n_feat):
            matrix = matrix + gram_in[k, local]
        gram[local] = matrix
        bound = jnp.max(jnp.sum(jnp.abs(matrix), axis=0, keepdims=True), axis=1, keepdims=True) * 1.0001
        low = 1.0 / bound
        scale = 2.0 / (bound + 1.0)
        inverse[local] = scale * (2.0 * eye - scale * matrix)
        lows.append(4.0 * low / ((1.0 + low) * (1.0 + low)))

    def newton(mm):
        def step(i, lows):
            scaled = [(2.0 / (1.0 + lows[k])) * inverse[k] for k in range(own)]
            products = [mm(gram[k], scaled[k]) for k in range(own)]
            for k in range(own):
                inverse[k] = 2.0 * scaled[k] - mm(scaled[k], products[k])
            return tuple(4.0 * low / ((1.0 + low) * (1.0 + low)) for low in lows)
        return step

    lows = lax.fori_loop(0, 5, newton(mm3), tuple(lows))
    lax.fori_loop(0, 2, newton(mm6), lows)

    duals[...] = jnp.zeros_like(duals)
    margins[...] = jnp.zeros_like(margins)
    weights[...] = jnp.zeros_like(weights)
    lane = lax.broadcasted_iota(jnp.int32, (1, LANES), 1)
    ones = jnp.ones((8, LANES), BF16)
    tiles = width // LANES

    def one_round(r, carry):
        mine = pl.ds(first, own)
        for k in range(own):
            residual = wanted[first + k] - duals[first + k] - margins[k]
            delta = mm6(jnp.broadcast_to(residual, (8, BLOCK)), inverse[k])
            d_buf[r, first + k] = delta[0:1]
        sends = []
        for k in range(1, n_feat):
            peer = (feat + k) % n_feat
            copy = to_feat(peer, d_buf.at[r, mine], d_buf.at[r, mine], d_ssem.at[r, peer], d_rsem.at[r, feat])
            copy.start()
            sends.append(copy)
        for k in range(1, n_feat):
            peer = (feat + k) % n_feat
            theirs = pl.ds(peer * own, own)
            to_feat(peer, d_buf.at[r, theirs], d_buf.at[r, theirs], d_ssem.at[r, peer], d_rsem.at[r, peer]).wait_recv()
        for copy in sends:
            copy.wait_send()

        for b in range(blocks):
            delta = d_buf[r, b]
            duals[b] = duals[b] + delta
            rounded = delta.astype(BF16).astype(F32)
            for h in range(0, BLOCK, LANES):
                tile = jnp.broadcast_to(rounded[:, h:h + LANES], (LANES, LANES))
                d_col[pl.ds(b * BLOCK + h, LANES), :] = tile.T

        def down(g, sums):
            at = pl.ds(pl.multiple_of(g * 16, 16), 16)
            column = d_col[at, :]
            result = []
            for c in range(tiles):
                term = phi[at, c * LANES:(c + 1) * LANES].astype(F32) * column
                result.append(sums[c] + (term[0:8] + term[8:16]))
            return tuple(result)

        sums = lax.fori_loop(0, rows // 16, down, tuple(jnp.zeros((8, LANES), F32) for _ in range(tiles)))
        for c in range(tiles):
            w_buf[r, samp, :, c * LANES:(c + 1) * LANES] = jnp.sum(sums[c], axis=0, keepdims=True) * step_scale
        sends = []
        for k in range(1, n_samp):
            peer = (samp + k) % n_samp
            copy = to_samp(peer, w_buf.at[r, samp], w_buf.at[r, samp], w_ssem.at[r, peer], w_rsem.at[r, samp])
            copy.start()
            sends.append(copy)
        for k in range(1, n_samp):
            peer = (samp + k) % n_samp
            to_samp(peer, w_buf.at[r, peer], w_buf.at[r, peer], w_ssem.at[r, peer], w_rsem.at[r, peer]).wait_recv()
        for copy in sends:
            copy.wait_send()

        change = w_buf[r, 0]
        for k in range(1, n_samp):
            change = change + w_buf[r, k]
        updated = weights[...] + change
        weights[...] = updated
        norm = jnp.sum(updated * updated, axis=1, keepdims=True)
        w_wide[...] = jnp.broadcast_to(updated.astype(BF16).astype(F32), (8, width))

        def across(g, carry):
            at = pl.ds(pl.multiple_of(g * 32, 32), 32)
            total = jnp.zeros((4, 8, LANES), F32)
            for c in range(tiles):
                term = phi[at, c * LANES:(c + 1) * LANES].astype(F32).reshape(4, 8, LANES)
                total = total + term * w_wide[:, c * LANES:(c + 1) * LANES][None]
            y[at, :] = total.reshape(32, LANES)
            return carry

        lax.fori_loop(0, rows // 32, across, 0)
        for b in range(blocks):
            high, middle, low = thirds(y[b * BLOCK:(b + 1) * BLOCK, :])
            m_send[r, b] = (nt(ones, high) + (nt(ones, middle) + nt(ones, low)))[0:1]
        for k in range(own):
            m_buf[r, feat, k] = m_send[r, first + k]
        sends = []
        for k in range(1, n_feat):
            peer = (feat + k) % n_feat
            copy = to_feat(peer, m_send.at[r, pl.ds(peer * own, own)], m_buf.at[r, feat], m_ssem.at[r, peer], m_rsem.at[r, feat])
            copy.start()
            sends.append(copy)
        for k in range(1, n_feat):
            peer = (feat + k) % n_feat
            to_feat(peer, m_buf.at[r, peer], m_buf.at[r, peer], m_ssem.at[r, peer], m_rsem.at[r, peer]).wait_recv()
        for copy in sends:
            copy.wait_send()

        squares = jnp.zeros((1, BLOCK), F32)
        dual_sum = jnp.zeros((1, BLOCK), F32)
        for k in range(own):
            value = m_buf[r, 0, k]
            for j in range(1, n_feat):
                value = value + m_buf[r, j, k]
            margins[k] = value
            goal, dual = wanted[first + k], duals[first + k]
            squares = squares + (value - goal) * (value - goal)
            dual_sum = dual_sum + (dual * goal - 0.5 * dual * dual)
        squares = jnp.sum(squares, axis=1, keepdims=True)
        dual_sum = jnp.sum(dual_sum, axis=1, keepdims=True)
        s_feat[feat, r] = jnp.where(lane == 0, squares, jnp.where(lane == 1, dual_sum, norm * (1.0 / n_samp)))
        return carry

    lax.fori_loop(0, ROUNDS, one_round, 0)

    sends = []
    for k in range(1, n_feat):
        peer = (feat + k) % n_feat
        copy = to_feat(peer, s_feat.at[feat], s_feat.at[feat], f_ssem.at[peer], f_rsem.at[feat])
        copy.start()
        sends.append(copy)

    w_out[...] = weights[...]
    restored = jnp.zeros((8, rows), F32)
    for b in range(blocks):
        restored = restored + nn(stacked(duals[b]), onehot[b * BLOCK:(b + 1) * BLOCK, :])
    duals_out[...] = unstacked(restored)

    for k in range(1, n_feat):
        peer = (feat + k) % n_feat
        to_feat(peer, s_feat.at[peer], s_feat.at[peer], f_ssem.at[peer], f_rsem.at[peer]).wait_recv()
    for copy in sends:
        copy.wait_send()
    total = s_feat[0]
    for k in range(1, n_feat):
        total = total + s_feat[k]
    s_samp[samp] = total
    sends = []
    for k in range(1, n_samp):
        peer = (samp + k) % n_samp
        copy = to_samp(peer, s_samp.at[samp], s_samp.at[samp], t_ssem.at[peer], t_rsem.at[samp])
        copy.start()
        sends.append(copy)
    for k in range(1, n_samp):
        peer = (samp + k) % n_samp
        to_samp(peer, s_samp.at[peer], s_samp.at[peer], t_ssem.at[peer], t_rsem.at[peer]).wait_recv()
    for copy in sends:
        copy.wait_send()
    total = s_samp[0]
    for k in range(1, n_samp):
        total = total + s_samp[k]
    penalty = 0.5 * ridge * total[:, :, 2:3]
    primal = total[:, :, 0:1] / (2.0 * sample_total) + penalty
    dual_value = total[:, :, 1:2] / sample_total - penalty
    obj_out[...] = jnp.where(lane[None] == 0, primal, dual_value)


def on_device(n_samp, n_feat, inputs, frequencies, phases, targets, block_order):
    rows = inputs.shape[0]
    width = frequencies.shape[1]
    blocks = rows // BLOCK
    own = blocks // n_feat
    dma = pltpu.SemaphoreType.DMA
    vmem = pl.BlockSpec(memory_space=pltpu.VMEM)
    weights, duals, objectives = pl.pallas_call(
        functools.partial(kernel, n_samp, n_feat),
        name="cocoa",
        out_shape=(
            jax.ShapeDtypeStruct((1, width), F32),
            jax.ShapeDtypeStruct((1, rows), F32),
            jax.ShapeDtypeStruct((ROUNDS, 1, LANES), F32),
        ),
        in_specs=[vmem] * 5,
        out_specs=(vmem, vmem, vmem),
        scratch_shapes=[
            pltpu.VMEM((rows, width), BF16),
            pltpu.VMEM((rows, rows), BF16),
            pltpu.VMEM((blocks, 1, BLOCK), F32),
            pltpu.VMEM((blocks, 1, BLOCK), F32),
            pltpu.VMEM((own, 1, BLOCK), F32),
            pltpu.VMEM((1, width), F32),
            pltpu.VMEM((8, width), F32),
            pltpu.VMEM((rows, LANES), F32),
            pltpu.VMEM((rows, LANES), F32),
            pltpu.VMEM((blocks, BLOCK, BLOCK), F32),
            pltpu.VMEM((n_feat, own, BLOCK, BLOCK), F32),
            pltpu.VMEM((own, BLOCK, BLOCK), F32),
            pltpu.VMEM((ROUNDS, blocks, 1, BLOCK), F32),
            pltpu.VMEM((ROUNDS, n_samp, 1, width), F32),
            pltpu.VMEM((ROUNDS, blocks, 1, BLOCK), F32),
            pltpu.VMEM((ROUNDS, n_feat, own, 1, BLOCK), F32),
            pltpu.VMEM((n_feat, ROUNDS, 1, LANES), F32),
            pltpu.VMEM((n_samp, ROUNDS, 1, LANES), F32),
            dma((n_feat, own)), dma((n_feat, own)),
            dma((ROUNDS, n_feat)), dma((ROUNDS, n_feat)),
            dma((ROUNDS, n_samp)), dma((ROUNDS, n_samp)),
            dma((ROUNDS, n_feat)), dma((ROUNDS, n_feat)),
            dma((n_feat,)), dma((n_feat,)),
            dma((n_samp,)), dma((n_samp,)),
        ],
        compiler_params=pltpu.CompilerParams(
            collective_id=0, has_side_effects=True, vmem_limit_bytes=60 * 2**20),
    )(inputs, frequencies, phases.reshape(1, width), targets.reshape(1, rows), block_order.reshape(rows, 1))
    return weights.reshape(width), duals.reshape(rows), objectives[:, 0, :2]


def solution(mesh):
    return jax.shard_map(
        functools.partial(on_device, mesh.shape["samp"], mesh.shape["feat"]),
        mesh=mesh,
        in_specs=(P("samp", None), P(None, "feat"), P("feat"), P("samp"), P("samp")),
        out_specs=(P("feat"), P("samp"), P()),
        check_vma=False,
    )
```

```python
import functools
import math

import jax
import jax.numpy as jnp
import numpy as np
from jax import lax
from jax.experimental import pallas as pl
from jax.experimental.pallas import tpu as pltpu
from jax.sharding import PartitionSpec as P

FEATURES = 16384
BLOCK = 256
ROUNDS = 4
LANES = 128
CHUNK = 512
PARTS = 2
MESH = pl.DeviceIdType.MESH
F32 = jnp.float32
BF16 = jnp.bfloat16


def cosine_coefficients():
    nodes = np.cos((np.arange(400) + 0.5) * np.pi / 400)
    square = (nodes + 1.0) / 8.0
    values = math.sqrt(2.0 / FEATURES) * np.cos(2.0 * np.pi * np.sqrt(square))
    fit = np.polynomial.chebyshev.Chebyshev.fit(square, values, 5, domain=[0.0, 0.25])
    return [float(c) for c in fit.convert(kind=np.polynomial.Polynomial).coef]


COEFS = cosine_coefficients()


def nn(a, b, precision=None):
    return lax.dot_general(a, b, (((1,), (0,)), ((), ())), precision=precision, preferred_element_type=F32)


def nt(a, b):
    return lax.dot_general(a, b, (((1,), (1,)), ((), ())), preferred_element_type=F32)


def halves(a):
    high = a.astype(BF16)
    return high, (a - high.astype(F32)).astype(BF16)


def thirds(a):
    high = a.astype(BF16)
    rest = a - high.astype(F32)
    middle = rest.astype(BF16)
    return high, middle, (rest - middle.astype(F32)).astype(BF16)


def mm3(a, b):
    a_high, a_low = halves(a)
    b_high, b_low = halves(b)
    return nn(a_high, b_high) + (nn(a_high, b_low) + nn(a_low, b_high))


def mm6(a, b):
    return nn(a, b, lax.Precision.HIGHEST)


def stacked(row):
    high, middle, low = (piece.astype(F32) for piece in thirds(row))
    at = lax.broadcasted_iota(jnp.int32, (8, row.shape[1]), 0)
    return jnp.where(at == 0, high, jnp.where(at == 1, middle, low)).astype(BF16)


def unstacked(rows):
    return rows[0:1] + rows[1:2] + rows[2:3]


def kernel(n_samp, n_feat, inputs, freqs, phases, targets, order, w_out, duals_out, obj_out,
           phi, onehot, wanted, duals, margins, weights, w_wide, y, gram, gram_in, inverse,
           d_buf, w_buf, m_send, m_buf, s_feat, s_samp,
           g_ssem, g_rsem, d_ssem, d_rsem, w_ssem, w_rsem, m_ssem, m_rsem, f_ssem, f_rsem, t_ssem, t_rsem):
    samp, feat = lax.axis_index("samp"), lax.axis_index("feat")
    rows, width = phi.shape
    blocks = rows // BLOCK
    own = blocks // n_feat
    sample_total = rows * n_samp
    ridge = 1.0 / BLOCK
    step_scale = BLOCK / sample_total
    first = feat * own

    barrier = pltpu.get_barrier_semaphore()
    for k in range(1, n_feat):
        pl.semaphore_signal(barrier, inc=1, device_id=(samp, (feat + k) % n_feat), device_id_type=MESH)
    for k in range(1, n_samp):
        pl.semaphore_signal(barrier, inc=1, device_id=((samp + k) % n_samp, feat), device_id_type=MESH)
    pl.semaphore_wait(barrier, n_feat + n_samp - 2)

    def to_feat(peer, src, dst, ssem, rsem):
        return pltpu.make_async_remote_copy(src_ref=src, dst_ref=dst, send_sem=ssem, recv_sem=rsem,
                                            device_id=(samp, peer), device_id_type=MESH)

    def to_samp(peer, src, dst, ssem, rsem):
        return pltpu.make_async_remote_copy(src_ref=src, dst_ref=dst, send_sem=ssem, recv_sem=rsem,
                                            device_id=(peer, feat), device_id_type=MESH)

    target_rows = stacked(targets[...])

    half = n_feat // 2
    chip, core = feat // 2, feat % 2

    def owner_of(k):
        return ((chip + 1 + k // 2) % half) * 2 + (core + 1 + k % 2) % 2

    def gram_copy(i):
        peer = owner_of(i // own)
        local = i % own
        return to_feat(peer, gram.at[peer * own + local], gram_in.at[feat, local],
                       g_ssem.at[peer, local], g_rsem.at[feat, local])

    def make_block(i, carry):
        block = owner_of(i // own) * own + i % own
        at = pl.ds(pl.multiple_of(block * BLOCK, BLOCK), BLOCK)
        position = lax.broadcasted_iota(jnp.int32, (LANES, rows), 1)
        strips = []
        for h in range(0, BLOCK, LANES):
            place = order[:, pl.ds(pl.multiple_of(block * BLOCK + h, LANES), LANES)].astype(F32)
            column = jnp.broadcast_to(place, (LANES, LANES)).T.astype(jnp.int32)[:, 0:1]
            strips.append(jnp.where(column == position, 1.0, 0.0).astype(BF16))
        hot = jnp.concatenate(strips, axis=0)
        onehot[at, :] = hot
        wanted[block] = unstacked(nt(target_rows, hot))
        picked = nt(hot, inputs[...]).astype(BF16)
        total = None
        for c in range(0, width, CHUNK):
            turns = nn(picked, freqs[:, c:c + CHUNK]) + phases[:, c:c + CHUNK]
            turns = turns * (0.5 / math.pi)
            turns = turns - jnp.floor(turns + 0.5)
            square = turns * turns
            value = COEFS[5] * square + COEFS[4]
            for coef in COEFS[3::-1]:
                value = value * square + coef
            part = value.astype(BF16)
            phi[at, c:c + CHUNK] = part
            term = nt(part, part)
            total = term if total is None else total + term

        @pl.when(i < blocks - own)
        def _():
            gram[block] = total
            gram_copy(i).start()

        @pl.when(i >= blocks - own)
        def _():
            gram_in[feat, i % own] = total

        return carry

    lax.fori_loop(0, blocks, make_block, 0)
    for i in range(blocks - own):
        peer = (feat + 1 + i // own) % n_feat
        copy = to_feat(peer, gram.at[peer * own + i % own], gram_in.at[peer, i % own],
                       g_ssem.at[peer, i % own], g_rsem.at[peer, i % own])
        copy.wait_recv()
        copy.wait_send()

    eye = jnp.where(lax.broadcasted_iota(jnp.int32, (BLOCK, BLOCK), 0)
                    == lax.broadcasted_iota(jnp.int32, (BLOCK, BLOCK), 1), 1.0, 0.0).astype(F32)
    lows = []
    for local in range(own):
        matrix = eye
        for k in range(n_feat):
            matrix = matrix + gram_in[k, local]
        gram[local] = matrix
        bound = jnp.max(jnp.sum(jnp.abs(matrix), axis=0, keepdims=True), axis=1, keepdims=True) * 1.0001
        low = 1.0 / bound
        scale = 2.0 / (bound + 1.0)
        inverse[local] = scale * (2.0 * eye - scale * matrix)
        lows.append(4.0 * low / ((1.0 + low) * (1.0 + low)))

    def newton(mm):
        def step(i, lows):
            scaled = [(2.0 / (1.0 + lows[k])) * inverse[k] for k in range(own)]
            products = [mm(gram[k], scaled[k]) for k in range(own)]
            for k in range(own):
                inverse[k] = 2.0 * scaled[k] - mm(scaled[k], products[k])
            return tuple(4.0 * low / ((1.0 + low) * (1.0 + low)) for low in lows)
        return step

    lows = lax.fori_loop(0, 5, newton(mm3), tuple(lows))
    lax.fori_loop(0, 2, newton(mm6), lows)

    duals[...] = jnp.zeros_like(duals)
    margins[...] = jnp.zeros_like(margins)
    weights[...] = jnp.zeros_like(weights)
    lane = lax.broadcasted_iota(jnp.int32, (1, LANES), 1)
    ones = jnp.ones((8, LANES), BF16)
    piece = width // PARTS
    step = min(CHUNK, piece)

    def one_round(r, carry):
        mine = pl.ds(first, own)
        for k in range(own):
            residual = wanted[first + k] - duals[first + k] - margins[k]
            delta = mm6(jnp.broadcast_to(residual, (8, BLOCK)), inverse[k])
            d_buf[r, first + k] = delta[0:1]
        sends = []
        for k in range(1, n_feat):
            peer = (feat + k) % n_feat
            copy = to_feat(peer, d_buf.at[r, mine], d_buf.at[r, mine], d_ssem.at[r, peer], d_rsem.at[r, feat])
            copy.start()
            sends.append(copy)
        for k in range(1, n_feat):
            peer = (feat + k) % n_feat
            theirs = pl.ds(peer * own, own)
            to_feat(peer, d_buf.at[r, theirs], d_buf.at[r, theirs], d_ssem.at[r, peer], d_rsem.at[r, peer]).wait_recv()
        for copy in sends:
            copy.wait_send()

        for b in range(blocks):
            delta = d_buf[r, b]
            duals[b] = duals[b] + delta

        moves = jnp.concatenate([jnp.broadcast_to(d_buf[r, b], (8, BLOCK)) for b in range(blocks)], axis=1).astype(BF16)
        sends = []
        for h in range(PARTS):
            def down(c, carry):
                w_buf[r, h, samp, c] = nn(moves, phi[:, pl.ds(pl.multiple_of(h * piece + c * step, step), step)])[0:1] * step_scale
                return carry

            lax.fori_loop(0, piece // step, down, 0)
            for k in range(1, n_samp):
                peer = (samp + k) % n_samp
                copy = to_samp(peer, w_buf.at[r, h, samp], w_buf.at[r, h, samp], w_ssem.at[r, h, peer], w_rsem.at[r, h, samp])
                copy.start()
                sends.append(copy)

        norm = jnp.zeros((1, 1), F32)
        for h in range(PARTS):
            for k in range(1, n_samp):
                peer = (samp + k) % n_samp
                to_samp(peer, w_buf.at[r, h, peer], w_buf.at[r, h, peer], w_ssem.at[r, h, peer], w_rsem.at[r, h, peer]).wait_recv()
            for c in range(piece // step):
                low = h * piece + c * step
                change = w_buf[r, h, 0, c]
                for k in range(1, n_samp):
                    change = change + w_buf[r, h, k, c]
                updated = weights[:, low:low + step] + change
                weights[:, low:low + step] = updated
                norm = norm + jnp.sum(updated * updated, axis=1, keepdims=True)
                w_wide[:, low:low + step] = jnp.broadcast_to(updated.astype(BF16).astype(F32), (8, step))
            start, split, stop = h * piece, h * piece + piece // 2, (h + 1) * piece
            rounded = w_wide[:, start:split].astype(BF16)

            def across(b, carry):
                at = pl.ds(pl.multiple_of(b * BLOCK, BLOCK), BLOCK)
                part = nt(rounded, phi[at, start:split])
                total = jnp.zeros((BLOCK // 8, 8, LANES), F32) if h == 0 else y[at, :].reshape(BLOCK // 8, 8, LANES)
                for c in range(split, stop, LANES):
                    term = phi[at, c:c + LANES].astype(F32).reshape(BLOCK // 8, 8, LANES)
                    total = total + term * w_wide[:, c:c + LANES][None]
                total = total.reshape(BLOCK, LANES)
                if h < PARTS - 1:
                    y[at, :] = total
                else:
                    high, middle, low = thirds(total)
                    part = part + (nt(ones, high) + (nt(ones, middle) + nt(ones, low)))
                m_send[r, b] = part[0:1] if h == 0 else m_send[r, b] + part[0:1]
                return carry

            lax.fori_loop(0, blocks, across, 0)
        for copy in sends:
            copy.wait_send()
        for k in range(own):
            m_buf[r, feat, k] = m_send[r, first + k]
        sends = []
        for k in range(1, n_feat):
            peer = (feat + k) % n_feat
            copy = to_feat(peer, m_send.at[r, pl.ds(peer * own, own)], m_buf.at[r, feat], m_ssem.at[r, peer], m_rsem.at[r, feat])
            copy.start()
            sends.append(copy)
        for k in range(1, n_feat):
            peer = (feat + k) % n_feat
            to_feat(peer, m_buf.at[r, peer], m_buf.at[r, peer], m_ssem.at[r, peer], m_rsem.at[r, peer]).wait_recv()
        for copy in sends:
            copy.wait_send()

        squares = jnp.zeros((1, BLOCK), F32)
        dual_sum = jnp.zeros((1, BLOCK), F32)
        for k in range(own):
            value = m_buf[r, 0, k]
            for j in range(1, n_feat):
                value = value + m_buf[r, j, k]
            margins[k] = value
            goal, dual = wanted[first + k], duals[first + k]
            squares = squares + (value - goal) * (value - goal)
            dual_sum = dual_sum + (dual * goal - 0.5 * dual * dual)
        squares = jnp.sum(squares, axis=1, keepdims=True)
        dual_sum = jnp.sum(dual_sum, axis=1, keepdims=True)
        s_feat[feat, r] = jnp.where(lane == 0, squares, jnp.where(lane == 1, dual_sum, norm * (1.0 / n_samp)))
        return carry

    lax.fori_loop(0, ROUNDS, one_round, 0)

    sends = []
    for k in range(1, n_feat):
        peer = (feat + k) % n_feat
        copy = to_feat(peer, s_feat.at[feat], s_feat.at[feat], f_ssem.at[peer], f_rsem.at[feat])
        copy.start()
        sends.append(copy)

    w_out[...] = weights[...]
    restored = jnp.zeros((8, rows), F32)
    for b in range(blocks):
        restored = restored + nn(stacked(duals[b]), onehot[b * BLOCK:(b + 1) * BLOCK, :])
    duals_out[...] = unstacked(restored)

    for k in range(1, n_feat):
        peer = (feat + k) % n_feat
        to_feat(peer, s_feat.at[peer], s_feat.at[peer], f_ssem.at[peer], f_rsem.at[peer]).wait_recv()
    for copy in sends:
        copy.wait_send()
    total = s_feat[0]
    for k in range(1, n_feat):
        total = total + s_feat[k]
    s_samp[samp] = total
    sends = []
    for k in range(1, n_samp):
        peer = (samp + k) % n_samp
        copy = to_samp(peer, s_samp.at[samp], s_samp.at[samp], t_ssem.at[peer], t_rsem.at[samp])
        copy.start()
        sends.append(copy)
    for k in range(1, n_samp):
        peer = (samp + k) % n_samp
        to_samp(peer, s_samp.at[peer], s_samp.at[peer], t_ssem.at[peer], t_rsem.at[peer]).wait_recv()
    for copy in sends:
        copy.wait_send()
    total = s_samp[0]
    for k in range(1, n_samp):
        total = total + s_samp[k]
    penalty = 0.5 * ridge * total[:, :, 2:3]
    primal = total[:, :, 0:1] / (2.0 * sample_total) + penalty
    dual_value = total[:, :, 1:2] / sample_total - penalty
    obj_out[...] = jnp.where(lane[None] == 0, primal, dual_value)


def on_device(n_samp, n_feat, inputs, frequencies, phases, targets, block_order):
    rows = inputs.shape[0]
    width = frequencies.shape[1]
    blocks = rows // BLOCK
    own = blocks // n_feat
    dma = pltpu.SemaphoreType.DMA
    vmem = pl.BlockSpec(memory_space=pltpu.VMEM)
    weights, duals, objectives = pl.pallas_call(
        functools.partial(kernel, n_samp, n_feat),
        name="cocoa",
        out_shape=(
            jax.ShapeDtypeStruct((1, width), F32),
            jax.ShapeDtypeStruct((1, rows), F32),
            jax.ShapeDtypeStruct((ROUNDS, 1, LANES), F32),
        ),
        in_specs=[vmem] * 5,
        out_specs=(vmem, vmem, vmem),
        scratch_shapes=[
            pltpu.VMEM((rows, width), BF16),
            pltpu.VMEM((rows, rows), BF16),
            pltpu.VMEM((blocks, 1, BLOCK), F32),
            pltpu.VMEM((blocks, 1, BLOCK), F32),
            pltpu.VMEM((own, 1, BLOCK), F32),
            pltpu.VMEM((1, width), F32),
            pltpu.VMEM((8, width), F32),
            pltpu.VMEM((rows, LANES), F32),
            pltpu.VMEM((blocks, BLOCK, BLOCK), F32),
            pltpu.VMEM((n_feat, own, BLOCK, BLOCK), F32),
            pltpu.VMEM((own, BLOCK, BLOCK), F32),
            pltpu.VMEM((ROUNDS, blocks, 1, BLOCK), F32),
            pltpu.VMEM((ROUNDS, PARTS, n_samp, width // PARTS // min(CHUNK, width // PARTS), 1, min(CHUNK, width // PARTS)), F32),
            pltpu.VMEM((ROUNDS, blocks, 1, BLOCK), F32),
            pltpu.VMEM((ROUNDS, n_feat, own, 1, BLOCK), F32),
            pltpu.VMEM((n_feat, ROUNDS, 1, LANES), F32),
            pltpu.VMEM((n_samp, ROUNDS, 1, LANES), F32),
            dma((n_feat, own)), dma((n_feat, own)),
            dma((ROUNDS, n_feat)), dma((ROUNDS, n_feat)),
            dma((ROUNDS, PARTS, n_samp)), dma((ROUNDS, PARTS, n_samp)),
            dma((ROUNDS, n_feat)), dma((ROUNDS, n_feat)),
            dma((n_feat,)), dma((n_feat,)),
            dma((n_samp,)), dma((n_samp,)),
        ],
        compiler_params=pltpu.CompilerParams(
            collective_id=0, has_side_effects=True, vmem_limit_bytes=60 * 2**20),
    )(inputs.T, frequencies, phases.reshape(1, width), targets.reshape(1, rows), block_order.reshape(1, rows))
    return weights.reshape(width), duals.reshape(rows), objectives[:, 0, :2]


def solution(mesh):
    return jax.shard_map(
        functools.partial(on_device, mesh.shape["samp"], mesh.shape["feat"]),
        mesh=mesh,
        in_specs=(P("samp", None), P(None, "feat"), P("feat"), P("samp"), P("samp")),
        out_specs=(P("feat"), P("samp"), P()),
        check_vma=False,
    )
```
